8 devices in a mesh: dp: 1 (over z), a: 2 (over y), b: 4 (over x, core).
Axes of the slice: x: 2, y: 2, z: 1, core: 2. Of those that a mesh axis runs over, the one named last changes fastest.
Arguments:
- x: bfloat16 [2048, 8192], P('dp', ('a', 'b'))
- w_gate: bfloat16 [8192, 32768], P('a', 'b')
- w_up: bfloat16 [8192, 32768], P('a', 'b')
- w_down: bfloat16 [32768, 8192], P('b', 'a')
Outputs:
- output: bfloat16 [2048, 8192], P('dp', ('a', 'b'))
All inputs are finite; a program needn't handle non-finite values.
Results may differ from the reference program's by a relative error of at most 0.016.
Values are sent between devices in bfloat16 or wider.
A program may use at most 2 GiB of HBM per device.

```python
import jax
import jax.numpy as jnp

ROWS = 2048
D = 8192
FF = 32768


def setup_inputs(seed: int = 0, part: int = 0) -> dict:
    kx, kg, ku, kd = jax.random.split(jax.random.key(seed), 4)
    drawn = {
        "x": jax.random.normal(jax.random.fold_in(kx, part), (ROWS, D), jnp.float32),
        "w_gate": jax.random.normal(kg, (D, FF), jnp.float32) * D**-0.5,
        "w_up": jax.random.normal(ku, (D, FF), jnp.float32) * D**-0.5,
        "w_down": jax.random.normal(kd, (FF, D), jnp.float32) * FF**-0.5,
    }
    return {k: v.astype(jnp.bfloat16) for k, v in drawn.items()}


def reference(x, w_gate, w_up, w_down):
    gate = jnp.dot(x, w_gate, preferred_element_type=jnp.float32)
    up = jnp.dot(x, w_up, preferred_element_type=jnp.float32)
    hidden = (jax.nn.silu(gate) * up).astype(jnp.bfloat16)
    return jnp.dot(hidden, w_down, preferred_element_type=jnp.float32).astype(jnp.bfloat16)
```

```python
import jax
import jax.numpy as jnp
from jax import lax
from jax.sharding import PartitionSpec as P

CHUNKS = (512, 1024, 512)


def solution(mesh):
    swap = [(0, 1), (1, 0)]

    def body(x, wg, wu, wd):
        mine = lax.axis_index("a")
        outs = []
        start = 0
        for rows in CHUNKS:
            half = rows // 2
            xc = lax.all_gather(x[start : start + rows], "b", axis=1, tiled=True)
            xt = lax.dynamic_slice_in_dim(xc, (1 - mine) * half, half, 0)
            xm = lax.dynamic_slice_in_dim(xc, mine * half, half, 0)
            gt = lax.ppermute(jnp.dot(xt, wg), "a", swap)
            ut = lax.ppermute(jnp.dot(xt, wu), "a", swap)
            gm = jnp.dot(xm, wg, preferred_element_type=jnp.float32)
            um = jnp.dot(xm, wu, preferred_element_type=jnp.float32)
            g = gm + gt.astype(jnp.float32)
            u = um + ut.astype(jnp.float32)
            h = (jax.nn.silu(g) * u).astype(jnp.bfloat16)
            ht = lax.ppermute(h, "a", swap)
            ym = jnp.dot(h, wd)
            yt = jnp.dot(ht, wd)
            lo = jnp.where(mine == 0, ym, yt)
            hi = jnp.where(mine == 0, yt, ym)
            y = jnp.concatenate([lo, hi], 0)
            outs.append(lax.psum_scatter(y, "b", scatter_dimension=1, tiled=True))
            start += rows
        return jnp.concatenate(outs, 0)

    return jax.shard_map(
        body,
        mesh=mesh,
        in_specs=(P("dp", ("a", "b")), P("a", "b"), P("a", "b"), P("b", "a")),
        out_specs=P("dp", ("a", "b")),
        check_vma=False,
    )
```

```python
import jax
import jax.numpy as jnp
from jax import lax
from jax.experimental import pallas as pl
from jax.experimental.pallas import tpu as pltpu
from jax.sharding import PartitionSpec as P

MESH = pl.DeviceIdType.MESH
F32 = jnp.float32
BF16 = jnp.bfloat16

U = 256
T = 256
GU, HS = 4, 4
LAG_H, LAG_Y = 3, 5
LAG_R = 6


def kernel(geom, x_ref, wg_ref, wu_ref, wd_ref, out_ref, xb, wb, wdb, own, gus, gur, hb, yacc, ysend, yrecv, yown, ost,
           xsend_sem, xrecv_sem, xloc_sem, w_sem, wd_sem, gu_send_sem, gu_recv_sem, h_send_sem, h_recv_sem,
           y_send_sem, y_recv_sem, o_sem, x_credit, gu_credit, h_credit, y_credit):
    units, pairs, nb, xcols, ocols = geom
    steps = units * pairs
    loads = pairs * (2 + (units - 2) // 2)
    dp, a, b = lax.axis_index("dp"), lax.axis_index("a"), lax.axis_index("b")
    across = (dp, 1 - a, b)

    def ahead(j):
        return (dp, a, lax.rem(b + j, nb))

    def behind(j):
        return (dp, a, lax.rem(b + nb - j, nb))

    def place(s):
        r = s - pairs
        last = s - (steps - pairs)
        head, tail = s < pairs, last >= 0
        two = 2 * pairs
        rc = jnp.maximum(r, 0)
        in_pass = lax.rem(rc, two)
        unit = jnp.where(head, 0, jnp.where(tail, units - 1, 1 + 2 * lax.div(rc, two) + lax.rem(in_pass, 2)))
        pair = jnp.where(head, s, jnp.where(tail, last, lax.div(in_pass, 2)))
        load = jnp.where(head, s, jnp.where(tail, loads - pairs + last, pairs + lax.div(rc, 2)))
        alone = jnp.logical_or(head, tail)
        first = jnp.logical_or(alone, lax.rem(rc, 2) == 0)
        final = jnp.logical_or(alone, lax.rem(rc, 2) == 1)
        return unit, pair, load, first, final

    def first_step(u):
        return 0 if u == 0 else steps - pairs if u == units - 1 else pairs + 2 * pairs * ((u - 1) // 2) + (u - 1) % 2

    def last_step(u):
        return pairs - 1 if u == 0 else steps - 1 if u == units - 1 else first_step(u) + 2 * (pairs - 1)

    def aligned(i, n):
        return pl.ds(pl.multiple_of(i * n, n), n)

    def w_copies(load, slot):
        pair = lax.rem(load, pairs)
        theirs, mine = aligned(2 * pair + 1 - a, T), aligned(2 * pair + a, T)
        return [
            pltpu.make_async_copy(ref.at[:, cols], wb.at[slot, i], w_sem.at[slot, i])
            for i, (ref, cols) in enumerate(((wg_ref, theirs), (wu_ref, theirs), (wg_ref, mine), (wu_ref, mine)))
        ]

    def wd_copy(load, slot):
        return pltpu.make_async_copy(
            wd_ref.at[aligned(lax.rem(load, pairs), 2 * T), :], wdb.at[slot], wd_sem.at[slot])

    def x_remote(u, j):
        slot = u % 4
        return pltpu.make_async_remote_copy(
            src_ref=x_ref.at[pl.ds(u * U, U), :], dst_ref=xb.at[slot, :, aligned(b, xcols)],
            send_sem=xsend_sem.at[slot, j - 1], recv_sem=xrecv_sem.at[slot, j - 1],
            device_id=ahead(j), device_id_type=MESH)

    def x_arrived(u, j):
        slot = u % 4
        return pltpu.make_async_remote_copy(
            src_ref=x_ref.at[pl.ds(u * U, U), :], dst_ref=xb.at[slot, :, aligned(lax.rem(b + nb - j, nb), xcols)],
            send_sem=xsend_sem.at[slot, j - 1], recv_sem=xrecv_sem.at[slot, j - 1],
            device_id=ahead(j), device_id_type=MESH)

    def x_local(u):
        slot = u % 4
        return pltpu.make_async_copy(
            x_ref.at[pl.ds(u * U, U), :], xb.at[slot, :, aligned(b, xcols)], xloc_sem.at[slot])

    def gu_copy(slot):
        return pltpu.make_async_remote_copy(
            src_ref=gus.at[slot], dst_ref=gur.at[slot], send_sem=gu_send_sem.at[slot], recv_sem=gu_recv_sem.at[slot],
            device_id=across, device_id_type=MESH)

    def h_copy(slot, half):
        return pltpu.make_async_remote_copy(
            src_ref=hb.at[slot, half], dst_ref=hb.at[slot, half], send_sem=h_send_sem.at[slot],
            recv_sem=h_recv_sem.at[slot], device_id=across, device_id_type=MESH)

    def y_copy(slot, j):
        return pltpu.make_async_remote_copy(
            src_ref=ysend.at[slot, j - 1], dst_ref=yrecv.at[slot, j - 1], send_sem=y_send_sem.at[slot, j - 1],
            recv_sem=y_recv_sem.at[slot, j - 1], device_id=ahead(j), device_id_type=MESH)

    def o_copy(u):
        return pltpu.make_async_copy(ost.at[u % 2], out_ref.at[pl.ds(u * U, U), :], o_sem.at[u % 2])

    def send_x(u):
        for j in range(1, nb):
            if u >= 4:
                x_remote(u - 4, j).wait_send()
                pl.semaphore_wait(x_credit.at[j - 1], 1)
            x_remote(u, j).start()
        x_local(u).start()

    def wait_x(u):
        x_local(u).wait()
        for j in range(1, nb):
            x_arrived(u, j).wait_recv()

    def free_x(u):
        if u + 4 < units:
            for j in range(1, nb):
                pl.semaphore_signal(x_credit.at[j - 1], inc=1, device_id=behind(j), device_id_type=MESH)

    def scatter_y(u):
        slot = u % 2
        for j in range(1, nb):
            if u >= 2:
                y_copy(slot, j).wait_send()
            ysend[slot, j - 1] = yacc[u % 2, :, aligned(lax.rem(b + j, nb), ocols)].astype(BF16)
        yown[slot] = yacc[u % 2, :, aligned(b, ocols)]
        for j in range(1, nb):
            if u >= 2:
                pl.semaphore_wait(y_credit.at[j - 1], 1)
            y_copy(slot, j).start()

    def sum_y(u):
        slot = u % 2
        if u >= 2:
            o_copy(u - 2).wait()
        for j in range(1, nb):
            y_copy(slot, j).wait_recv()
        total = yown[slot]
        for j in range(1, nb):
            total += yrecv[slot, j - 1].astype(F32)
        ost[slot] = total.astype(BF16)
        o_copy(u).start()
        if u + 2 < units:
            for j in range(1, nb):
                pl.semaphore_signal(y_credit.at[j - 1], inc=1, device_id=behind(j), device_id_type=MESH)

    for copy in w_copies(0, 0):
        copy.start()

    barrier = pltpu.get_barrier_semaphore()
    for peer in [across] + [ahead(j) for j in range(1, nb)]:
        pl.semaphore_signal(barrier, inc=1, device_id=peer, device_id_type=MESH)
    pl.semaphore_wait(barrier, nb)

    send_x(0)
    wd_copy(0, 0).start()
    for copy in w_copies(1, 1):
        copy.start()
    wd_copy(1, 1).start()

    def first_matmuls(s):
        unit, pair, load, first, final = place(s)
        slot, wslot, xslot = lax.rem(s, GU), lax.rem(load, 2), lax.rem(unit, 4)

        @pl.when(first)
        def _():
            for copy in w_copies(load, wslot):
                copy.wait()

        for u in range(units):
            @pl.when(s == first_step(u))
            def _():
                wait_x(u)
                if u == 0:
                    for later in range(1, min(4, units)):
                        send_x(later)

        @pl.when(s >= GU)
        def _():
            gu_copy(slot).wait_send()

        rows = xb.at[xslot]
        for i in range(2):
            gus[slot, i] = jnp.dot(rows[...], wb[wslot, i], preferred_element_type=F32).astype(BF16)

        @pl.when(s >= GU)
        def _():
            pl.semaphore_wait(gu_credit, 1)

        gu_copy(slot).start()
        for i in range(2):
            own[slot, i] = jnp.dot(rows[...], wb[wslot, 2 + i], preferred_element_type=F32)

        @pl.when(jnp.logical_and(final, load + 2 < loads))
        def _():
            for copy in w_copies(load + 2, wslot):
                copy.start()

        for u in range(units):
            @pl.when(s == last_step(u))
            def _():
                free_x(u)

    def hidden(s):
        slot, hslot = lax.rem(s, GU), lax.rem(s, HS)

        @pl.when(s >= HS)
        def _():
            h_copy(hslot, a).wait_send()

        gu_copy(slot).wait_recv()
        g = own[slot, 0] + gur[slot, 0].astype(F32)
        u = own[slot, 1] + gur[slot, 1].astype(F32)
        hb[hslot, a] = (jax.nn.silu(g) * u).astype(BF16)

        @pl.when(s + GU < steps)
        def _():
            pl.semaphore_signal(gu_credit, inc=1, device_id=across, device_id_type=MESH)

        @pl.when(s >= HS)
        def _():
            pl.semaphore_wait(h_credit, 1)

        h_copy(hslot, a).start()

    def last_matmul(s):
        unit, pair, load, first, final = place(s)
        hslot, wslot, yslot = lax.rem(s, HS), lax.rem(load, 2), lax.rem(unit, 2)

        @pl.when(first)
        def _():
            wd_copy(load, wslot).wait()

        h_copy(hslot, 1 - a).wait_recv()

        @pl.when(pair == 0)
        def _():
            yacc[yslot] = jnp.zeros_like(yacc[yslot])

        yacc[yslot] += (
            jnp.dot(hb[hslot, 0], wdb[wslot, :T], preferred_element_type=F32)
            + jnp.dot(hb[hslot, 1], wdb[wslot, T:], preferred_element_type=F32))

        @pl.when(s + HS < steps)
        def _():
            pl.semaphore_signal(h_credit, inc=1, device_id=across, device_id_type=MESH)

        @pl.when(jnp.logical_and(final, load + 2 < loads))
        def _():
            wd_copy(load + 2, wslot).start()

        for u in range(units):
            @pl.when(s == last_step(u))
            def _():
                scatter_y(u)
            if u < units - 1:
                @pl.when(s == last_step(u) + LAG_R)
                def _():
                    sum_y(u)

    @pl.loop(0, steps + LAG_Y)
    def _(s):
        @pl.when(s < steps)
        def _():
            first_matmuls(s)

        for u in range(4, units):
            @pl.when(s == last_step(u - 4) + 3)
            def _():
                send_x(u)

        @pl.when(jnp.logical_and(s >= LAG_H, s < steps + LAG_H))
        def _():
            hidden(s - LAG_H)

        @pl.when(s >= LAG_Y)
        def _():
            last_matmul(s - LAG_Y)

    sum_y(units - 1)
    for u in (units - 2, units - 1):
        o_copy(u).wait()
        for j in range(1, nb):
            y_copy(u % 2, j).wait_send()
    for u in range(units - 4, units):
        for j in range(1, nb):
            x_remote(u, j).wait_send()
    for s in range(steps - GU, steps):
        gu_copy(s % GU).wait_send()
    for s in range(steps - HS, steps):
        h_copy(s % HS, a).wait_send()


def solution(mesh):
    nb = mesh.shape["b"]

    def body(x, wg, wu, wd):
        rows, xcols = x.shape
        depth, hidden = wg.shape
        outs = wd.shape[1]
        ocols = outs // nb
        units, pairs = rows // U, hidden // (2 * T)
        geom = (units, pairs, nb, xcols, ocols)
        dma, reg = pltpu.SemaphoreType.DMA, pltpu.SemaphoreType.REGULAR
        return pl.pallas_call(
            lambda *refs: kernel(geom, *refs),
            out_shape=jax.ShapeDtypeStruct((rows, ocols), BF16),
            in_specs=[pl.BlockSpec(memory_space=pl.ANY)] * 4,
            out_specs=pl.BlockSpec(memory_space=pl.ANY),
            scratch_shapes=[
                pltpu.VMEM((4, U, depth), BF16),
                pltpu.VMEM((2, 4, depth, T), BF16),
                pltpu.VMEM((2, 2 * T, outs), BF16),
                pltpu.VMEM((GU, 2, U, T), F32),
                pltpu.VMEM((GU, 2, U, T), BF16),
                pltpu.VMEM((GU, 2, U, T), BF16),
                pltpu.VMEM((HS, 2, U, T), BF16),
                pltpu.VMEM((2, U, outs), F32),
                pltpu.VMEM((2, nb - 1, U, ocols), BF16),
                pltpu.VMEM((2, nb - 1, U, ocols), BF16),
                pltpu.VMEM((2, U, ocols), F32),
                pltpu.VMEM((2, U, ocols), BF16),
                dma((4, nb - 1)), dma((4, nb - 1)), dma((4,)),
                dma((2, 4)), dma((2,)),
                dma((GU,)), dma((GU,)), dma((HS,)), dma((HS,)),
                dma((2, nb - 1)), dma((2, nb - 1)), dma((2,)),
                reg((nb - 1,)), reg, reg, reg((nb - 1,)),
            ],
            compiler_params=pltpu.CompilerParams(
                collective_id=0, has_side_effects=True, vmem_limit_bytes=67043328),
            cost_estimate=pl.CostEstimate(
                flops=6 * rows * depth * hidden, bytes_accessed=10 * depth * hidden * 3, transcendentals=rows * hidden),
            name="gated_mlp",
        )(x, wg, wu, wd)

    return jax.shard_map(
        body,
        mesh=mesh,
        in_specs=(P("dp", ("a", "b")), P("a", "b"), P("a", "b"), P("b", "a")),
        out_specs=P("dp", ("a", "b")),
        check_vma=False,
    )
```

```python
import jax
import jax.numpy as jnp
from jax import lax
from jax.experimental import pallas as pl
from jax.experimental.pallas import tpu as pltpu
from jax.sharding import PartitionSpec as P

MESH = pl.DeviceIdType.MESH
F32 = jnp.float32
BF16 = jnp.bfloat16

U = 128
T = 256
GU, HS = 4, 4
LAG_H, LAG_Y = 3, 5
LAG_R = 6


def kernel(geom, x_ref, wg_ref, wu_ref, wd_ref, out_ref, xb, wb, wdb, own, gus, gur, hb, yacc, ysend, yrecv, yown, ost,
           xsend_sem, xrecv_sem, xloc_sem, w_sem, wd_sem, gu_send_sem, gu_recv_sem, h_send_sem, h_recv_sem,
           y_send_sem, y_recv_sem, o_sem, x_credit, gu_credit, h_credit, y_credit):
    units, pairs, nb, xcols, ocols = geom
    steps = units * pairs
    loads = pairs * (2 + (units - 2) // 2)
    dp, a, b = lax.axis_index("dp"), lax.axis_index("a"), lax.axis_index("b")
    across = (dp, 1 - a, b)

    def ahead(j):
        return (dp, a, lax.rem(b + j, nb))

    def behind(j):
        return (dp, a, lax.rem(b + nb - j, nb))

    def place(s):
        r = s - pairs
        last = s - (steps - pairs)
        head, tail = s < pairs, last >= 0
        two = 2 * pairs
        rc = jnp.maximum(r, 0)
        in_pass = lax.rem(rc, two)
        unit = jnp.where(head, 0, jnp.where(tail, units - 1, 1 + 2 * lax.div(rc, two) + lax.rem(in_pass, 2)))
        pair = jnp.where(head, s, jnp.where(tail, last, lax.div(in_pass, 2)))
        load = jnp.where(head, s, jnp.where(tail, loads - pairs + last, pairs + lax.div(rc, 2)))
        alone = jnp.logical_or(head, tail)
        first = jnp.logical_or(alone, lax.rem(rc, 2) == 0)
        final = jnp.logical_or(alone, lax.rem(rc, 2) == 1)
        return unit, pair, load, first, final

    def first_step(u):
        return 0 if u == 0 else steps - pairs if u == units - 1 else pairs + 2 * pairs * ((u - 1) // 2) + (u - 1) % 2

    def last_step(u):
        return pairs - 1 if u == 0 else steps - 1 if u == units - 1 else first_step(u) + 2 * (pairs - 1)

    def aligned(i, n):
        return pl.ds(pl.multiple_of(i * n, n), n)

    def w_copies(load, slot):
        pair = lax.rem(load, pairs)
        theirs, mine = aligned(2 * pair + 1 - a, T), aligned(2 * pair + a, T)
        return [
            pltpu.make_async_copy(ref.at[:, cols], wb.at[slot, i], w_sem.at[slot, i])
            for i, (ref, cols) in enumerate(((wg_ref, theirs), (wu_ref, theirs), (wg_ref, mine), (wu_ref, mine)))
        ]

    def wd_copy(load, slot):
        return pltpu.make_async_copy(
            wd_ref.at[aligned(lax.rem(load, pairs), 2 * T), :], wdb.at[slot], wd_sem.at[slot])

    def x_remote(u, j):
        slot = u % 4
        return pltpu.make_async_remote_copy(
            src_ref=x_ref.at[pl.ds(u * U, U), :], dst_ref=xb.at[slot, :, aligned(b, xcols)],
            send_sem=xsend_sem.at[slot, j - 1], recv_sem=xrecv_sem.at[slot, j - 1],
            device_id=ahead(j), device_id_type=MESH)

    def x_arrived(u, j):
        slot = u % 4
        return pltpu.make_async_remote_copy(
            src_ref=x_ref.at[pl.ds(u * U, U), :], dst_ref=xb.at[slot, :, aligned(lax.rem(b + nb - j, nb), xcols)],
            send_sem=xsend_sem.at[slot, j - 1], recv_sem=xrecv_sem.at[slot, j - 1],
            device_id=ahead(j), device_id_type=MESH)

    def x_local(u):
        slot = u % 4
        return pltpu.make_async_copy(
            x_ref.at[pl.ds(u * U, U), :], xb.at[slot, :, aligned(b, xcols)], xloc_sem.at[slot])

    def gu_copy(slot):
        return pltpu.make_async_remote_copy(
            src_ref=gus.at[slot], dst_ref=gur.at[slot], send_sem=gu_send_sem.at[slot], recv_sem=gu_recv_sem.at[slot],
            device_id=across, device_id_type=MESH)

    def h_copy(slot, half):
        return pltpu.make_async_remote_copy(
            src_ref=hb.at[slot, half], dst_ref=hb.at[slot, half], send_sem=h_send_sem.at[slot],
            recv_sem=h_recv_sem.at[slot], device_id=across, device_id_type=MESH)

    def y_copy(slot, j):
        return pltpu.make_async_remote_copy(
            src_ref=ysend.at[slot, j - 1], dst_ref=yrecv.at[slot, j - 1], send_sem=y_send_sem.at[slot, j - 1],
            recv_sem=y_recv_sem.at[slot, j - 1], device_id=ahead(j), device_id_type=MESH)

    def o_copy(u):
        return pltpu.make_async_copy(ost.at[u % 2], out_ref.at[pl.ds(u * U, U), :], o_sem.at[u % 2])

    def send_x(u):
        for j in range(1, nb):
            if u >= 4:
                x_remote(u - 4, j).wait_send()
                pl.semaphore_wait(x_credit.at[j - 1], 1)
            x_remote(u, j).start()
        x_local(u).start()

    def wait_x(u):
        x_local(u).wait()
        for j in range(1, nb):
            x_arrived(u, j).wait_recv()

    def free_x(u):
        if u + 4 < units:
            for j in range(1, nb):
                pl.semaphore_signal(x_credit.at[j - 1], inc=1, device_id=behind(j), device_id_type=MESH)

    def scatter_y(u):
        slot = u % 2
        for j in range(1, nb):
            if u >= 2:
                y_copy(slot, j).wait_send()
            ysend[slot, j - 1] = yacc[u % 2, :, aligned(lax.rem(b + j, nb), ocols)].astype(BF16)
        yown[slot] = yacc[u % 2, :, aligned(b, ocols)]
        for j in range(1, nb):
            if u >= 2:
                pl.semaphore_wait(y_credit.at[j - 1], 1)
            y_copy(slot, j).start()

    def sum_y(u):
        slot = u % 2
        for j in range(1, nb):
            y_copy(slot, j).wait_recv()
        total = yown[slot]
        for j in range(1, nb):
            total += yrecv[slot, j - 1].astype(F32)
        out_ref[pl.ds(u * U, U), :] = total.astype(BF16)
        if u + 2 < units:
            for j in range(1, nb):
                pl.semaphore_signal(y_credit.at[j - 1], inc=1, device_id=behind(j), device_id_type=MESH)

    for copy in w_copies(0, 0):
        copy.start()

    barrier = pltpu.get_barrier_semaphore()
    for peer in [across] + [ahead(j) for j in range(1, nb)]:
        pl.semaphore_signal(barrier, inc=1, device_id=peer, device_id_type=MESH)
    pl.semaphore_wait(barrier, nb)

    send_x(0)
    wd_copy(0, 0).start()
    for copy in w_copies(1, 1):
        copy.start()
    wd_copy(1, 1).start()

    def first_matmuls(s):
        unit, pair, load, first, final = place(s)
        slot, wslot, xslot = lax.rem(s, GU), lax.rem(load, 2), lax.rem(unit, 4)

        @pl.when(first)
        def _():
            for copy in w_copies(load, wslot):
                copy.wait()

        for u in range(units):
            @pl.when(s == first_step(u))
            def _():
                wait_x(u)

        @pl.when(s >= GU)
        def _():
            gu_copy(slot).wait_send()

        rows = xb.at[xslot]
        for i in range(2):
            gus[slot, i] = jnp.dot(rows[...], wb[wslot, i], preferred_element_type=F32).astype(BF16)

        @pl.when(s >= GU)
        def _():
            pl.semaphore_wait(gu_credit, 1)

        gu_copy(slot).start()
        for i in range(2):
            own[slot, i] = jnp.dot(rows[...], wb[wslot, 2 + i], preferred_element_type=F32)

        @pl.when(jnp.logical_and(final, load + 2 < loads))
        def _():
            for copy in w_copies(load + 2, wslot):
                copy.start()

        for u in range(units):
            @pl.when(s == last_step(u))
            def _():
                free_x(u)

    def hidden(s):
        slot, hslot = lax.rem(s, GU), lax.rem(s, HS)

        @pl.when(s >= HS)
        def _():
            h_copy(hslot, a).wait_send()

        gu_copy(slot).wait_recv()
        g = own[slot, 0] + gur[slot, 0].astype(F32)
        u = own[slot, 1] + gur[slot, 1].astype(F32)
        hb[hslot, a] = (jax.nn.silu(g) * u).astype(BF16)

        @pl.when(s + GU < steps)
        def _():
            pl.semaphore_signal(gu_credit, inc=1, device_id=across, device_id_type=MESH)

        @pl.when(s >= HS)
        def _():
            pl.semaphore_wait(h_credit, 1)

        h_copy(hslot, a).start()

    def last_matmul(s):
        unit, pair, load, first, final = place(s)
        hslot, wslot, yslot = lax.rem(s, HS), lax.rem(load, 2), lax.rem(unit, 2)

        @pl.when(first)
        def _():
            wd_copy(load, wslot).wait()

        h_copy(hslot, 1 - a).wait_recv()

        @pl.when(pair == 0)
        def _():
            yacc[yslot] = jnp.zeros_like(yacc[yslot])

        yacc[yslot] += (
            jnp.dot(hb[hslot, 0], wdb[wslot, :T], preferred_element_type=F32)
            + jnp.dot(hb[hslot, 1], wdb[wslot, T:], preferred_element_type=F32))

        @pl.when(s + HS < steps)
        def _():
            pl.semaphore_signal(h_credit, inc=1, device_id=across, device_id_type=MESH)

        @pl.when(jnp.logical_and(final, load + 2 < loads))
        def _():
            wd_copy(load + 2, wslot).start()

        for u in range(units):
            @pl.when(s == last_step(u))
            def _():
                scatter_y(u)
            if u < units - 1:
                @pl.when(s == last_step(u) + LAG_R)
                def _():
                    sum_y(u)

    @pl.loop(0, steps + LAG_Y)
    def _(s):
        @pl.when(s < steps)
        def _():
            first_matmuls(s)

        for u in range(1, units):
            @pl.when(s == (2 * u if u < 4 else last_step(u - 4) + 3))
            def _():
                send_x(u)

        @pl.when(jnp.logical_and(s >= LAG_H, s < steps + LAG_H))
        def _():
            hidden(s - LAG_H)

        @pl.when(s >= LAG_Y)
        def _():
            last_matmul(s - LAG_Y)

    sum_y(units - 1)
    for u in (units - 2, units - 1):
        for j in range(1, nb):
            y_copy(u % 2, j).wait_send()
    for u in range(units - 4, units):
        for j in range(1, nb):
            x_remote(u, j).wait_send()
    for s in range(steps - GU, steps):
        gu_copy(s % GU).wait_send()
    for s in range(steps - HS, steps):
        h_copy(s % HS, a).wait_send()


def solution(mesh):
    nb = mesh.shape["b"]

    def body(x, wg, wu, wd):
        rows, xcols = x.shape
        depth, hidden = wg.shape
        outs = wd.shape[1]
        ocols = outs // nb
        units, pairs = rows // U, hidden // (2 * T)
        geom = (units, pairs, nb, xcols, ocols)
        dma, reg = pltpu.SemaphoreType.DMA, pltpu.SemaphoreType.REGULAR
        return pl.pallas_call(
            lambda *refs: kernel(geom, *refs),
            out_shape=pltpu.VMEM((rows, ocols), BF16),
            in_specs=[pl.BlockSpec(memory_space=pl.ANY)] * 4,
            out_specs=pl.BlockSpec(memory_space=pltpu.VMEM),
            scratch_shapes=[
                pltpu.VMEM((4, U, depth), BF16),
                pltpu.VMEM((2, 4, depth, T), BF16),
                pltpu.VMEM((2, 2 * T, outs), BF16),
                pltpu.VMEM((GU, 2, U, T), F32),
                pltpu.VMEM((GU, 2, U, T), BF16),
                pltpu.VMEM((GU, 2, U, T), BF16),
                pltpu.VMEM((HS, 2, U, T), BF16),
                pltpu.VMEM((2, U, outs), F32),
                pltpu.VMEM((2, nb - 1, U, ocols), BF16),
                pltpu.VMEM((2, nb - 1, U, ocols), BF16),
                pltpu.VMEM((2, U, ocols), F32),
                pltpu.VMEM((2, U, ocols), BF16),
                dma((4, nb - 1)), dma((4, nb - 1)), dma((4,)),
                dma((2, 4)), dma((2,)),
                dma((GU,)), dma((GU,)), dma((HS,)), dma((HS,)),
                dma((2, nb - 1)), dma((2, nb - 1)), dma((2,)),
                reg((nb - 1,)), reg, reg, reg((nb - 1,)),
            ],
            compiler_params=pltpu.CompilerParams(
                collective_id=0, has_side_effects=True, vmem_limit_bytes=58 * 1024 * 1024),
            cost_estimate=pl.CostEstimate(
                flops=6 * rows * depth * hidden, bytes_accessed=10 * depth * hidden * 3, transcendentals=rows * hidden),
            name="gated_mlp",
        )(x, wg, wu, wd)

    return jax.shard_map(
        body,
        mesh=mesh,
        in_specs=(P("dp", ("a", "b")), P("a", "b"), P("a", "b"), P("b", "a")),
        out_specs=P("dp", ("a", "b")),
        check_vma=False,
    )
```

```python
import jax
import jax.numpy as jnp
from jax import lax
from jax.experimental import pallas as pl
from jax.experimental.pallas import tpu as pltpu
from jax.sharding import PartitionSpec as P

MESH = pl.DeviceIdType.MESH
F32 = jnp.float32
BF16 = jnp.bfloat16

U = 128
T = 256
GU, HS = 4, 4
LAG_H, LAG_Y = 3, 5
LAG_R = 13


def kernel(geom, x_ref, wg_ref, wu_ref, wd_ref, out_ref, xb, wb, wdb, own, gus, gur, hb, yacc, ysend, yrecv, yown, ost,
           xsend_sem, xrecv_sem, xloc_sem, w_sem, wd_sem, gu_send_sem, gu_recv_sem, h_send_sem, h_recv_sem,
           y_send_sem, y_recv_sem, o_sem, x_credit, gu_credit, h_credit, y_credit):
    units, pairs, nb, xcols, ocols = geom
    steps = units * pairs
    loads = pairs * (2 + (units - 2) // 2)
    dp, a, b = lax.axis_index("dp"), lax.axis_index("a"), lax.axis_index("b")
    across = (dp, 1 - a, b)

    def ahead(j):
        return (dp, a, lax.rem(b + j, nb))

    def behind(j):
        return (dp, a, lax.rem(b + nb - j, nb))

    def place(s):
        r = s - pairs
        last = s - (steps - pairs)
        head, tail = s < pairs, last >= 0
        two = 2 * pairs
        rc = jnp.maximum(r, 0)
        in_pass = lax.rem(rc, two)
        unit = jnp.where(head, 0, jnp.where(tail, units - 1, 1 + 2 * lax.div(rc, two) + lax.rem(in_pass, 2)))
        pair = jnp.where(head, s, jnp.where(tail, last, lax.div(in_pass, 2)))
        load = jnp.where(head, s, jnp.where(tail, loads - pairs + last, pairs + lax.div(rc, 2)))
        alone = jnp.logical_or(head, tail)
        first = jnp.logical_or(alone, lax.rem(rc, 2) == 0)
        final = jnp.logical_or(alone, lax.rem(rc, 2) == 1)
        return unit, pair, load, first, final

    def first_step(u):
        return 0 if u == 0 else steps - pairs if u == units - 1 else pairs + 2 * pairs * ((u - 1) // 2) + (u - 1) % 2

    def last_step(u):
        return pairs - 1 if u == 0 else steps - 1 if u == units - 1 else first_step(u) + 2 * (pairs - 1)

    def aligned(i, n):
        return pl.ds(pl.multiple_of(i * n, n), n)

    def w_copies(load, slot):
        pair = lax.rem(load, pairs)
        theirs, mine = aligned(2 * pair + 1 - a, T), aligned(2 * pair + a, T)
        return [
            pltpu.make_async_copy(ref.at[:, cols], wb.at[slot, i], w_sem.at[slot, i])
            for i, (ref, cols) in enumerate(((wg_ref, theirs), (wu_ref, theirs), (wg_ref, mine), (wu_ref, mine)))
        ]

    def wd_copy(load, slot):
        return pltpu.make_async_copy(
            wd_ref.at[aligned(lax.rem(load, pairs), 2 * T), :], wdb.at[slot], wd_sem.at[slot])

    def x_remote(u, j):
        slot = u % 4
        return pltpu.make_async_remote_copy(
            src_ref=x_ref.at[pl.ds(u * U, U), :], dst_ref=xb.at[slot, :, aligned(b, xcols)],
            send_sem=xsend_sem.at[slot, j - 1], recv_sem=xrecv_sem.at[slot, j - 1],
            device_id=ahead(j), device_id_type=MESH)

    def x_arrived(u, j):
        slot = u % 4
        return pltpu.make_async_remote_copy(
            src_ref=x_ref.at[pl.ds(u * U, U), :], dst_ref=xb.at[slot, :, aligned(lax.rem(b + nb - j, nb), xcols)],
            send_sem=xsend_sem.at[slot, j - 1], recv_sem=xrecv_sem.at[slot, j - 1],
            device_id=ahead(j), device_id_type=MESH)

    def x_local(u):
        slot = u % 4
        return pltpu.make_async_copy(
            x_ref.at[pl.ds(u * U, U), :], xb.at[slot, :, aligned(b, xcols)], xloc_sem.at[slot])

    def gu_copy(slot):
        return pltpu.make_async_remote_copy(
            src_ref=gus.at[slot], dst_ref=gur.at[slot], send_sem=gu_send_sem.at[slot], recv_sem=gu_recv_sem.at[slot],
            device_id=across, device_id_type=MESH)

    def h_copy(slot, half):
        return pltpu.make_async_remote_copy(
            src_ref=hb.at[slot, half], dst_ref=hb.at[slot, half], send_sem=h_send_sem.at[slot],
            recv_sem=h_recv_sem.at[slot], device_id=across, device_id_type=MESH)

    def y_copy(slot, j):
        return pltpu.make_async_remote_copy(
            src_ref=ysend.at[slot, j - 1], dst_ref=yrecv.at[slot, j - 1], send_sem=y_send_sem.at[slot, j - 1],
            recv_sem=y_recv_sem.at[slot, j - 1], device_id=ahead(j), device_id_type=MESH)

    def o_copy(u):
        return pltpu.make_async_copy(ost.at[u % 2], out_ref.at[pl.ds(u * U, U), :], o_sem.at[u % 2])

    def send_x(u):
        for j in range(1, nb):
            if u >= 4:
                x_remote(u - 4, j).wait_send()
                pl.semaphore_wait(x_credit.at[j - 1], 1)
            x_remote(u, j).start()
        x_local(u).start()

    def wait_x(u):
        x_local(u).wait()
        for j in range(1, nb):
            x_arrived(u, j).wait_recv()

    def free_x(u):
        if u + 4 < units:
            for j in range(1, nb):
                pl.semaphore_signal(x_credit.at[j - 1], inc=1, device_id=behind(j), device_id_type=MESH)

    def scatter_y(u):
        slot = u % 2
        for j in range(1, nb):
            if u >= 2:
                y_copy(slot, j).wait_send()
            ysend[slot, j - 1] = yacc[u % 2, :, aligned(lax.rem(b + j, nb), ocols)].astype(BF16)
        yown[slot] = yacc[u % 2, :, aligned(b, ocols)]
        for j in range(1, nb):
            if u >= 2:
                pl.semaphore_wait(y_credit.at[j - 1], 1)
            y_copy(slot, j).start()

    def sum_y(u):
        slot = u % 2
        for j in range(1, nb):
            y_copy(slot, j).wait_recv()
        total = yown[slot]
        for j in range(1, nb):
            total += yrecv[slot, j - 1].astype(F32)
        out_ref[pl.ds(u * U, U), :] = total.astype(BF16)
        if u + 2 < units:
            for j in range(1, nb):
                pl.semaphore_signal(y_credit.at[j - 1], inc=1, device_id=behind(j), device_id_type=MESH)

    for copy in w_copies(0, 0):
        copy.start()

    barrier = pltpu.get_barrier_semaphore()
    for peer in [across] + [ahead(j) for j in range(1, nb)]:
        pl.semaphore_signal(barrier, inc=1, device_id=peer, device_id_type=MESH)
    pl.semaphore_wait(barrier, nb)

    send_x(0)
    wd_copy(0, 0).start()
    for copy in w_copies(1, 1):
        copy.start()
    wd_copy(1, 1).start()

    def first_matmuls(s):
        unit, pair, load, first, final = place(s)
        slot, wslot, xslot = lax.rem(s, GU), lax.rem(load, 2), lax.rem(unit, 4)

        @pl.when(first)
        def _():
            for copy in w_copies(load, wslot):
                copy.wait()

        for u in range(units):
            @pl.when(s == first_step(u))
            def _():
                wait_x(u)

        @pl.when(s >= GU)
        def _():
            gu_copy(slot).wait_send()

        rows = xb.at[xslot]
        for i in range(2):
            gus[slot, i] = jnp.dot(rows[...], wb[wslot, i], preferred_element_type=F32).astype(BF16)

        @pl.when(s >= GU)
        def _():
            pl.semaphore_wait(gu_credit, 1)

        gu_copy(slot).start()
        for i in range(2):
            own[slot, i] = jnp.dot(rows[...], wb[wslot, 2 + i], preferred_element_type=F32)

        @pl.when(jnp.logical_and(final, load + 2 < loads))
        def _():
            for copy in w_copies(load + 2, wslot):
                copy.start()

        for u in range(units):
            @pl.when(s == last_step(u))
            def _():
                free_x(u)

    def hidden(s):
        slot, hslot = lax.rem(s, GU), lax.rem(s, HS)

        @pl.when(s >= HS)
        def _():
            h_copy(hslot, a).wait_send()

        gu_copy(slot).wait_recv()
        g = own[slot, 0] + gur[slot, 0].astype(F32)
        u = own[slot, 1] + gur[slot, 1].astype(F32)
        hb[hslot, a] = (jax.nn.silu(g) * u).astype(BF16)

        @pl.when(s + GU < steps)
        def _():
            pl.semaphore_signal(gu_credit, inc=1, device_id=across, device_id_type=MESH)

        @pl.when(s >= HS)
        def _():
            pl.semaphore_wait(h_credit, 1)

        h_copy(hslot, a).start()

    def last_matmul(s):
        unit, pair, load, first, final = place(s)
        hslot, wslot, yslot = lax.rem(s, HS), lax.rem(load, 2), lax.rem(unit, 2)

        @pl.when(first)
        def _():
            wd_copy(load, wslot).wait()

        h_copy(hslot, 1 - a).wait_recv()

        @pl.when(pair == 0)
        def _():
            yacc[yslot] = jnp.zeros_like(yacc[yslot])

        yacc[yslot] += (
            jnp.dot(hb[hslot, 0], wdb[wslot, :T], preferred_element_type=F32)
            + jnp.dot(hb[hslot, 1], wdb[wslot, T:], preferred_element_type=F32))

        @pl.when(s + HS < steps)
        def _():
            pl.semaphore_signal(h_credit, inc=1, device_id=across, device_id_type=MESH)

        @pl.when(jnp.logical_and(final, load + 2 < loads))
        def _():
            wd_copy(load + 2, wslot).start()

        for u in range(units):
            @pl.when(s == last_step(u))
            def _():
                scatter_y(u)
            if u < units - 1:
                @pl.when(s == last_step(u) + LAG_R)
                def _():
                    sum_y(u)

    @pl.loop(0, steps + LAG_Y)
    def _(s):
        @pl.when(s < steps)
        def _():
            first_matmuls(s)

        for u in range(1, units):
            @pl.when(s == (2 * u if u < 4 else last_step(u - 4) + 3))
            def _():
                send_x(u)

        @pl.when(jnp.logical_and(s >= LAG_H, s < steps + LAG_H))
        def _():
            hidden(s - LAG_H)

        @pl.when(s >= LAG_Y)
        def _():
            last_matmul(s - LAG_Y)

    sum_y(units - 1)
    for u in (units - 2, units - 1):
        for j in range(1, nb):
            y_copy(u % 2, j).wait_send()
    for u in range(units - 4, units):
        for j in range(1, nb):
            x_remote(u, j).wait_send()
    for s in range(steps - GU, steps):
        gu_copy(s % GU).wait_send()
    for s in range(steps - HS, steps):
        h_copy(s % HS, a).wait_send()


def solution(mesh):
    nb = mesh.shape["b"]

    def body(x, wg, wu, wd):
        rows, xcols = x.shape
        depth, hidden = wg.shape
        outs = wd.shape[1]
        ocols = outs // nb
        units, pairs = rows // U, hidden // (2 * T)
        geom = (units, pairs, nb, xcols, ocols)
        dma, reg = pltpu.SemaphoreType.DMA, pltpu.SemaphoreType.REGULAR
        return pl.pallas_call(
            lambda *refs: kernel(geom, *refs),
            out_shape=pltpu.VMEM((rows, ocols), BF16),
            in_specs=[pl.BlockSpec(memory_space=pl.ANY)] * 4,
            out_specs=pl.BlockSpec(memory_space=pltpu.VMEM),
            scratch_shapes=[
                pltpu.VMEM((4, U, depth), BF16),
                pltpu.VMEM((2, 4, depth, T), BF16),
                pltpu.VMEM((2, 2 * T, outs), BF16),
                pltpu.VMEM((GU, 2, U, T), F32),
                pltpu.VMEM((GU, 2, U, T), BF16),
                pltpu.VMEM((GU, 2, U, T), BF16),
                pltpu.VMEM((HS, 2, U, T), BF16),
                pltpu.VMEM((2, U, outs), F32),
                pltpu.VMEM((2, nb - 1, U, ocols), BF16),
                pltpu.VMEM((2, nb - 1, U, ocols), BF16),
                pltpu.VMEM((2, U, ocols), F32),
                pltpu.VMEM((2, U, ocols), BF16),
                dma((4, nb - 1)), dma((4, nb - 1)), dma((4,)),
                dma((2, 4)), dma((2,)),
                dma((GU,)), dma((GU,)), dma((HS,)), dma((HS,)),
                dma((2, nb - 1)), dma((2, nb - 1)), dma((2,)),
                reg((nb - 1,)), reg, reg, reg((nb - 1,)),
            ],
            compiler_params=pltpu.CompilerParams(
                collective_id=0, has_side_effects=True, vmem_limit_bytes=58 * 1024 * 1024),
            cost_estimate=pl.CostEstimate(
                flops=6 * rows * depth * hidden, bytes_accessed=10 * depth * hidden * 3, transcendentals=rows * hidden),
            name="gated_mlp",
        )(x, wg, wu, wd)

    return jax.shard_map(
        body,
        mesh=mesh,
        in_specs=(P("dp", ("a", "b")), P("a", "b"), P("a", "b"), P("b", "a")),
        out_specs=P("dp", ("a", "b")),
        check_vma=False,
    )
```

```python
import jax
import jax.numpy as jnp
from jax import lax
from jax.experimental import pallas as pl
from jax.experimental.pallas import tpu as pltpu
from jax.sharding import PartitionSpec as P

MESH = pl.DeviceIdType.MESH
F32 = jnp.float32
BF16 = jnp.bfloat16

U = 128
T = 256
GU, HS = 4, 4
LAG_H, LAG_Y = 3, 5
LAG_R = 13


def kernel(geom, x_ref, wg_ref, wu_ref, wd_ref, out_ref, xb, wb, wdb, own, gus, gur, hb, yacc, ysend, yrecv, yown, ost,
           xsend_sem, xrecv_sem, xloc_sem, w_sem, wd_sem, gu_send_sem, gu_recv_sem, h_send_sem, h_recv_sem,
           y_send_sem, y_recv_sem, o_sem, x_credit, gu_credit, h_credit, y_credit):
    units, pairs, nb, xcols, ocols = geom
    steps = units * pairs
    loads = pairs * (2 + (units - 2) // 2)
    dp, a, b = lax.axis_index("dp"), lax.axis_index("a"), lax.axis_index("b")
    across = (dp, 1 - a, b)

    def ahead(j):
        return (dp, a, lax.rem(b + j, nb))

    def behind(j):
        return (dp, a, lax.rem(b + nb - j, nb))

    def place(s):
        r = s - pairs
        last = s - (steps - pairs)
        head, tail = s < pairs, last >= 0
        two = 2 * pairs
        rc = jnp.maximum(r, 0)
        in_pass = lax.rem(rc, two)
        unit = jnp.where(head, 0, jnp.where(tail, units - 1, 1 + 2 * lax.div(rc, two) + lax.rem(in_pass, 2)))
        pair = jnp.where(head, s, jnp.where(tail, last, lax.div(in_pass, 2)))
        load = jnp.where(head, s, jnp.where(tail, loads - pairs + last, pairs + lax.div(rc, 2)))
        alone = jnp.logical_or(head, tail)
        first = jnp.logical_or(alone, lax.rem(rc, 2) == 0)
        final = jnp.logical_or(alone, lax.rem(rc, 2) == 1)
        return unit, pair, load, first, final

    def first_step(u):
        return 0 if u == 0 else steps - pairs if u == units - 1 else pairs + 2 * pairs * ((u - 1) // 2) + (u - 1) % 2

    def last_step(u):
        return pairs - 1 if u == 0 else steps - 1 if u == units - 1 else first_step(u) + 2 * (pairs - 1)

    def aligned(i, n):
        return pl.ds(pl.multiple_of(i * n, n), n)

    def w_copies(load, slot):
        pair = lax.rem(load, pairs)
        theirs, mine = aligned(2 * pair + 1 - a, T), aligned(2 * pair + a, T)
        return [
            pltpu.make_async_copy(ref.at[:, cols], wb.at[slot, i], w_sem.at[slot, i])
            for i, (ref, cols) in enumerate(((wg_ref, theirs), (wu_ref, theirs), (wg_ref, mine), (wu_ref, mine)))
        ]

    def wd_copy(load, slot):
        return pltpu.make_async_copy(
            wd_ref.at[aligned(lax.rem(load, pairs), 2 * T), :], wdb.at[slot], wd_sem.at[slot])

    def x_remote(u, j):
        slot = u % 4
        return pltpu.make_async_remote_copy(
            src_ref=x_ref.at[pl.ds(u * U, U), :], dst_ref=xb.at[slot, :, aligned(b, xcols)],
            send_sem=xsend_sem.at[slot, j - 1], recv_sem=xrecv_sem.at[slot, j - 1],
            device_id=ahead(j), device_id_type=MESH)

    def x_arrived(u, j):
        slot = u % 4
        return pltpu.make_async_remote_copy(
            src_ref=x_ref.at[pl.ds(u * U, U), :], dst_ref=xb.at[slot, :, aligned(lax.rem(b + nb - j, nb), xcols)],
            send_sem=xsend_sem.at[slot, j - 1], recv_sem=xrecv_sem.at[slot, j - 1],
            device_id=ahead(j), device_id_type=MESH)

    def x_local(u):
        slot = u % 4
        return pltpu.make_async_copy(
            x_ref.at[pl.ds(u * U, U), :], xb.at[slot, :, aligned(b, xcols)], xloc_sem.at[slot])

    def gu_copy(slot):
        return pltpu.make_async_remote_copy(
            src_ref=gus.at[slot], dst_ref=gur.at[slot], send_sem=gu_send_sem.at[slot], recv_sem=gu_recv_sem.at[slot],
            device_id=across, device_id_type=MESH)

    def h_copy(slot, half):
        return pltpu.make_async_remote_copy(
            src_ref=hb.at[slot, half], dst_ref=hb.at[slot, half], send_sem=h_send_sem.at[slot],
            recv_sem=h_recv_sem.at[slot], device_id=across, device_id_type=MESH)

    def y_copy(slot, j):
        return pltpu.make_async_remote_copy(
            src_ref=ysend.at[slot, j - 1], dst_ref=yrecv.at[slot, j - 1], send_sem=y_send_sem.at[slot, j - 1],
            recv_sem=y_recv_sem.at[slot, j - 1], device_id=ahead(j), device_id_type=MESH)

    def o_copy(u):
        return pltpu.make_async_copy(ost.at[u % 2], out_ref.at[pl.ds(u * U, U), :], o_sem.at[u % 2])

    def send_x(u):
        for j in range(1, nb):
            if u >= 4:
                x_remote(u - 4, j).wait_send()
                pl.semaphore_wait(x_credit.at[j - 1], 1)
            x_remote(u, j).start()
        x_local(u).start()

    def wait_x(u):
        x_local(u).wait()
        for j in range(1, nb):
            x_arrived(u, j).wait_recv()

    def free_x(u):
        if u + 4 < units:
            for j in range(1, nb):
                pl.semaphore_signal(x_credit.at[j - 1], inc=1, device_id=behind(j), device_id_type=MESH)

    def scatter_y(unit, finish):
        slot = lax.rem(unit, 2)
        dests = (1, 2, 3)

        def block(j):
            cols = aligned(lax.rem(b + j, nb), ocols)
            return yacc[slot, :, cols] + finish(cols)

        for i, j in enumerate(dests):
            @pl.when(unit >= 2)
            def _():
                y_copy(slot, j).wait_send()

            ysend[slot, j - 1] = block(j).astype(BF16)
            if i:
                start_y(unit, slot, dests[i - 1])
        yown[slot] = block(0)
        start_y(unit, slot, dests[-1])

    def start_y(unit, slot, j):
        @pl.when(unit >= 2)
        def _():
            pl.semaphore_wait(y_credit.at[j - 1], 1)

        y_copy(slot, j).start()

    def sum_y(u):
        slot = u % 2
        for j in range(1, nb):
            y_copy(slot, j).wait_recv()
        total = yown[slot]
        for j in range(1, nb):
            total += yrecv[slot, j - 1].astype(F32)
        out_ref[pl.ds(u * U, U), :] = total.astype(BF16)
        if u + 2 < units:
            for j in range(1, nb):
                pl.semaphore_signal(y_credit.at[j - 1], inc=1, device_id=behind(j), device_id_type=MESH)

    for copy in w_copies(0, 0):
        copy.start()

    barrier = pltpu.get_barrier_semaphore()
    for peer in [across] + [ahead(j) for j in range(1, nb)]:
        pl.semaphore_signal(barrier, inc=1, device_id=peer, device_id_type=MESH)
    pl.semaphore_wait(barrier, nb)

    send_x(0)
    wd_copy(0, 0).start()
    for copy in w_copies(1, 1):
        copy.start()
    wd_copy(1, 1).start()

    def first_matmuls(s):
        unit, pair, load, first, final = place(s)
        slot, wslot, xslot = lax.rem(s, GU), lax.rem(load, 2), lax.rem(unit, 4)

        @pl.when(first)
        def _():
            for copy in w_copies(load, wslot):
                copy.wait()

        for u in range(units):
            @pl.when(s == first_step(u))
            def _():
                wait_x(u)

        @pl.when(s >= GU)
        def _():
            gu_copy(slot).wait_send()

        rows = xb.at[xslot]
        for i in range(2):
            gus[slot, i] = jnp.dot(rows[...], wb[wslot, i], preferred_element_type=F32).astype(BF16)

        @pl.when(s >= GU)
        def _():
            pl.semaphore_wait(gu_credit, 1)

        gu_copy(slot).start()
        for i in range(2):
            own[slot, i] = jnp.dot(rows[...], wb[wslot, 2 + i], preferred_element_type=F32)

        @pl.when(jnp.logical_and(final, load + 2 < loads))
        def _():
            for copy in w_copies(load + 2, wslot):
                copy.start()

        for u in range(units):
            @pl.when(s == last_step(u))
            def _():
                free_x(u)

    def hidden(s):
        slot, hslot = lax.rem(s, GU), lax.rem(s, HS)

        @pl.when(s >= HS)
        def _():
            h_copy(hslot, a).wait_send()

        gu_copy(slot).wait_recv()
        g = own[slot, 0] + gur[slot, 0].astype(F32)
        u = own[slot, 1] + gur[slot, 1].astype(F32)
        hb[hslot, a] = (jax.nn.silu(g) * u).astype(BF16)

        @pl.when(s + GU < steps)
        def _():
            pl.semaphore_signal(gu_credit, inc=1, device_id=across, device_id_type=MESH)

        @pl.when(s >= HS)
        def _():
            pl.semaphore_wait(h_credit, 1)

        h_copy(hslot, a).start()

    def last_matmul(s):
        unit, pair, load, first, final = place(s)
        hslot, wslot, yslot = lax.rem(s, HS), lax.rem(load, 2), lax.rem(unit, 2)

        @pl.when(first)
        def _():
            wd_copy(load, wslot).wait()

        @pl.when(pair == 0)
        def _():
            yacc[yslot] = jnp.zeros_like(yacc[yslot])

        yacc[yslot] += jnp.dot(hb[hslot, a], wdb[wslot, aligned(a, T)], preferred_element_type=F32)
        h_copy(hslot, 1 - a).wait_recv()

        def theirs(cols):
            return jnp.dot(hb[hslot, 1 - a], wdb[wslot, aligned(1 - a, T), cols], preferred_element_type=F32)

        @pl.when(pair < pairs - 1)
        def _():
            yacc[yslot] += theirs(slice(None))

        @pl.when(pair == pairs - 1)
        def _():
            scatter_y(unit, theirs)

        @pl.when(s + HS < steps)
        def _():
            pl.semaphore_signal(h_credit, inc=1, device_id=across, device_id_type=MESH)

        @pl.when(jnp.logical_and(final, load + 2 < loads))
        def _():
            wd_copy(load + 2, wslot).start()

        for u in range(units):
            if u < units - 1:
                @pl.when(s == last_step(u) + LAG_R)
                def _():
                    sum_y(u)

    @pl.loop(0, steps + LAG_Y)
    def _(s):
        @pl.when(s < steps)
        def _():
            first_matmuls(s)

        for u in range(1, units):
            @pl.when(s == (2 * u if u < 4 else last_step(u - 4) + 3))
            def _():
                send_x(u)

        @pl.when(jnp.logical_and(s >= LAG_H, s < steps + LAG_H))
        def _():
            hidden(s - LAG_H)

        @pl.when(s >= LAG_Y)
        def _():
            last_matmul(s - LAG_Y)

    sum_y(units - 1)
    for u in (units - 2, units - 1):
        for j in range(1, nb):
            y_copy(u % 2, j).wait_send()
    for u in range(units - 4, units):
        for j in range(1, nb):
            x_remote(u, j).wait_send()
    for s in range(steps - GU, steps):
        gu_copy(s % GU).wait_send()
    for s in range(steps - HS, steps):
        h_copy(s % HS, a).wait_send()


def solution(mesh):
    nb = mesh.shape["b"]

    def body(x, wg, wu, wd):
        rows, xcols = x.shape
        depth, hidden = wg.shape
        outs = wd.shape[1]
        ocols = outs // nb
        units, pairs = rows // U, hidden // (2 * T)
        geom = (units, pairs, nb, xcols, ocols)
        dma, reg = pltpu.SemaphoreType.DMA, pltpu.SemaphoreType.REGULAR
        return pl.pallas_call(
            lambda *refs: kernel(geom, *refs),
            out_shape=pltpu.VMEM((rows, ocols), BF16),
            in_specs=[pl.BlockSpec(memory_space=pl.ANY)] * 4,
            out_specs=pl.BlockSpec(memory_space=pltpu.VMEM),
            scratch_shapes=[
                pltpu.VMEM((4, U, depth), BF16),
                pltpu.VMEM((2, 4, depth, T), BF16),
                pltpu.VMEM((2, 2 * T, outs), BF16),
                pltpu.VMEM((GU, 2, U, T), F32),
                pltpu.VMEM((GU, 2, U, T), BF16),
                pltpu.VMEM((GU, 2, U, T), BF16),
                pltpu.VMEM((HS, 2, U, T), BF16),
                pltpu.VMEM((2, U, outs), F32),
                pltpu.VMEM((2, nb - 1, U, ocols), BF16),
                pltpu.VMEM((2, nb - 1, U, ocols), BF16),
                pltpu.VMEM((2, U, ocols), F32),
                pltpu.VMEM((2, U, ocols), BF16),
                dma((4, nb - 1)), dma((4, nb - 1)), dma((4,)),
                dma((2, 4)), dma((2,)),
                dma((GU,)), dma((GU,)), dma((HS,)), dma((HS,)),
                dma((2, nb - 1)), dma((2, nb - 1)), dma((2,)),
                reg((nb - 1,)), reg, reg, reg((nb - 1,)),
            ],
            compiler_params=pltpu.CompilerParams(
                collective_id=0, has_side_effects=True, vmem_limit_bytes=58 * 1024 * 1024),
            cost_estimate=pl.CostEstimate(
                flops=6 * rows * depth * hidden, bytes_accessed=10 * depth * hidden * 3, transcendentals=rows * hidden),
            name="gated_mlp",
        )(x, wg, wu, wd)

    return jax.shard_map(
        body,
        mesh=mesh,
        in_specs=(P("dp", ("a", "b")), P("a", "b"), P("a", "b"), P("b", "a")),
        out_specs=P("dp", ("a", "b")),
        check_vma=False,
    )
```
